256 devices in a mesh: band: 4 (over x, y), tm: 64 (over z, core).
Axes of the slice: x: 2, y: 2, z: 32, core: 2. Of those that a mesh axis runs over, the one named last changes fastest.
The devices are a block of a 4x8x32 slice.
Arguments:
- voltages: bfloat16 [32, 2, 512, 16384], P('band', None, None, 'tm'), parts along dimension 0, may hold values from -12 to 12
- antenna_flags: int32 [128, 32], P('tm', 'band'), parts along dimension 1, may hold values from -2147483648 to 2147483647, as said below
- owned_tile: int32 [64], replicated, may hold values from 0 to 63, each once
Outputs:
- visibility: float32 [512, 32, 2, 512], P('tm', 'band'), parts along dimension 1
The draws below stay inside these ranges and needn't reach their ends.
There are 4 independent parts, one for each index of `band`. The reference program is written for one: setup_inputs(seed, part) draws one part's arguments, and reference() takes and returns one part's arrays. A program takes and returns all parts, laid end to end along the dimension named above; an argument that names none is the same for every part. Nothing has to cross between parts.
Inputs may be any that keep to these rules, and one draw needn't show every extreme that they name: `antenna_flags`: bit b of word w of sub-integration s is 1 where the samples of both polarisations of antenna 32 * w + b are good in that sub-integration of 128 samples, 0 where flagged; all 32 bits of a word are used; some antennas may be flagged in every sub-integration. A permutation: the index k of tm holds the baseline rows of tile owned_tile[k].
All inputs are finite; a program needn't handle non-finite values.
Results may differ from the reference program's by a relative error of at most 0.0003.
Values sent between devices are 32-bit elements; how exact they have to be, the bound alone decides.
A program may use at most 128 MiB of HBM per device.

```python
import math
import jax
import jax.numpy as jnp
from jax import lax

ANTENNAS = 256
INPUTS = 512
FLAG_WORDS = 8
CHANS = 8
SAMPLES_DEV = 256
SUB_LEN = 128
SUBS = 128
TIME = 16384
TILES = 64
N_TM = 64


def gains(key, lowest, highest):
    key_amplitude, key_phase = jax.random.split(key)
    amplitude = jnp.exp(jax.random.uniform(key_amplitude, (INPUTS,), jnp.float32, math.log(lowest), math.log(highest)))
    phase = jax.random.uniform(key_phase, (INPUTS,), jnp.float32, -math.pi, math.pi)
    return (amplitude * jnp.cos(phase), amplitude * jnp.sin(phase))


def source_term(key, lowest, highest):
    key_sky, key_gain = jax.random.split(key)
    sky = jax.random.normal(key_sky, (CHANS, 2, 1, TIME), jnp.float32)
    gain_real, gain_imag = gains(key_gain, lowest, highest)
    gain_real = gain_real[None, :, None]
    gain_imag = gain_imag[None, :, None]
    real_term = gain_real * sky[:, 0] - gain_imag * sky[:, 1]
    imag_term = gain_real * sky[:, 1] + gain_imag * sky[:, 0]
    return jnp.stack([real_term, imag_term], axis=1)


def draw_voltages(key, part):
    key_first = jax.random.fold_in(jax.random.fold_in(key, 11), 0)
    key_noise = jax.random.fold_in(jax.random.fold_in(key, 11), 2)
    noise = jax.random.normal(key_noise, (CHANS, 2, INPUTS, TIME), jnp.float32)
    signal = source_term(key_first, 0.5, 2.0)
    return jnp.clip(signal + noise, -12.0, 12.0).astype(jnp.bfloat16)


def draw_antenna_flags(key, part):
    key_rolled, key_dead = jax.random.split(jax.random.fold_in(key, 23))
    sub_position = jnp.arange(SUBS, dtype=jnp.int32)[:, None]
    threshold = 30 + 60 * sub_position // max(SUBS - 1, 1)
    rolled = jax.random.randint(key_rolled, (SUBS, ANTENNAS), 0, 100)
    ranking = jax.random.permutation(key_dead, ANTENNAS)
    alive = ranking >= max(1, ANTENNAS // 64)
    bits = jnp.where(alive[None, :] & (rolled < threshold), 1, 0).astype(jnp.int32)
    bits = bits.reshape(SUBS, FLAG_WORDS, 32)
    shifts = jnp.arange(32, dtype=jnp.int32)
    return jnp.sum(jnp.left_shift(bits, shifts[None, None, :]), axis=-1, dtype=jnp.int32)


def setup_inputs(seed: int = 0, part: int = 0) -> dict:
    key_list = jax.random.split(jax.random.key(seed), 4)
    own_keys = jax.random.split(jax.random.fold_in(key_list[3], part), 4)
    voltages = draw_voltages(jax.random.fold_in(jax.random.fold_in(key_list[3], part), 71), part)
    antenna_flags = draw_antenna_flags(jax.random.fold_in(jax.random.fold_in(key_list[3], part), 71), part)
    owned_tile = jax.random.permutation(key_list[2], TILES).astype(jnp.int32)
    return {"voltages": voltages, "antenna_flags": antenna_flags, "owned_tile": owned_tile}


def unpack_flags(words):
    shifts = jnp.arange(32, dtype=jnp.int32)
    bits = jnp.bitwise_and(jnp.right_shift(words[:, :, None], shifts[None, None, :]), 1)
    return bits.reshape(words.shape[0], words.shape[1] * 32).astype(jnp.int32)


def reference(voltages, antenna_flags, owned_tile):
    channels = voltages.shape[0]
    inputs = voltages.shape[2]
    block_rows = inputs // N_TM
    good = unpack_flags(antenna_flags)
    input_flags = jnp.repeat(good, 2, axis=1)
    sample_flags = jnp.repeat(input_flags.T, SUB_LEN, axis=1).astype(jnp.bfloat16)
    masked = voltages * sample_flags[None, None]

    def add_block(running, block_index):
        segment = lax.dynamic_slice_in_dim(masked, block_index * SAMPLES_DEV, SAMPLES_DEV, 3).astype(jnp.float32)
        real_part = segment[:, 0]
        imag_part = segment[:, 1]
        right_side = jnp.concatenate([real_part, imag_part], axis=-1)
        left_side = jnp.stack([right_side, jnp.concatenate([imag_part, -real_part], axis=-1)], axis=1)
        return running + jnp.einsum("ckiu,cju->ckij", left_side, right_side), None

    initial = jnp.zeros((channels, 2, inputs, inputs), jnp.float32)
    gram = lax.scan(add_block, initial, jnp.arange(N_TM, dtype=jnp.int32))[0]
    counts = SUB_LEN * jnp.dot(good.T, good)
    row_index = (owned_tile[:, None] * block_rows + jnp.arange(block_rows, dtype=jnp.int32)[None, :]).reshape(-1)
    pair_counts = jnp.repeat(jnp.repeat(counts, 2, axis=0), 2, axis=1)[row_index]
    ordered = jnp.transpose(gram[:, :, row_index, :], (2, 0, 1, 3))
    return ordered / jnp.maximum(pair_counts, 1).astype(jnp.float32)[:, None, None, :]
```

```python
import functools

import jax
import jax.numpy as jnp
from jax import lax
from jax.experimental import pallas as pl
from jax.experimental.pallas import tpu as pltpu
from jax.sharding import PartitionSpec as P

MESH = pl.DeviceIdType.MESH
F32 = jnp.float32
BF16 = jnp.bfloat16
LANES = 128
WORD = 32


def dot_nt(a, b):
    return lax.dot_general(a, b, (((1,), (1,)), ((), ())), preferred_element_type=F32)


def bit_of(words, shifts):
    return jnp.bitwise_and(lax.shift_right_logical(words, shifts), 1)


def iota(shape, dim):
    return lax.broadcasted_iota(jnp.int32, shape, dim)


def swap_chunks(blocks, width):
    count = len(blocks)
    lanes = count * width
    blocks = list(blocks)
    stride = count // 2
    while stride:
        chunk = lax.div(iota(blocks[0].shape, 1), width)
        low = jnp.bitwise_and(chunk, stride) == 0
        for i in range(count):
            if i & stride:
                continue
            a, b = blocks[i], blocks[i + stride]
            blocks[i] = jnp.where(low, a, pltpu.roll(b, stride * width, 1))
            blocks[i + stride] = jnp.where(low, pltpu.roll(a, lanes - stride * width, 1), b)
        stride //= 2
    return blocks


def kernel(
    n, tiles, flags, v_hbm, out, *refs
):
    channels = v_hbm.shape[0]
    vbuf = refs[:channels]
    (
        mask, x, onehot, ring_m, ring_e, sib_m, sib_e, own_m, own_e, snd_m, snd_e, turned, exch, final, arrived,
        vsem, ring_send, ring_recv, sib_send, sib_recv, exch_send, exch_recv, fin_send, fin_recv,
    ) = refs[channels:]
    parts, _, block, samples = vbuf[0].shape
    half_ch = channels // 2
    subs = flags.shape[0]
    sub_len = samples // subs
    rows = 2 * block
    inputs = n * rows
    hops = n // 2
    window = hops * rows
    ants = block // 2
    per_word = WORD // ants
    group = parts * rows

    me = lax.axis_index("tm")
    z = lax.div(me, 2)
    core = lax.rem(me, 2)
    sigma = 1 - 2 * core
    other = 1 - core

    def wrap(k):
        return lax.rem(k + 2 * n, n)

    def device(chip, which):
        return {"tm": 2 * chip + which}

    ahead = (device(wrap(z + sigma), core), device(wrap(z - sigma), core))
    sibling = device(z, other)

    def v_copy(c):
        return pltpu.make_async_copy(v_hbm.at[c], vbuf[c], vsem.at[c])

    for c in range(channels):
        v_copy(c).start()

    barrier = pltpu.get_barrier_semaphore()
    for peer in (*ahead, sibling):
        pl.semaphore_signal(barrier, inc=1, device_id=peer, device_id_type=MESH)

    row = iota((rows, LANES), 0)
    upper = row >= block

    def make_mask(q, _):
        t0, t1 = tiles[2 * q], tiles[2 * q + 1]
        shift = jnp.where(upper, lax.rem(t1, per_word) * ants, lax.rem(t0, per_word) * ants) + lax.div(lax.rem(row, block), 2)
        for s in range(subs):
            words = jnp.where(upper, flags[s, lax.div(t1, per_word)], flags[s, lax.div(t0, per_word)])
            mask[s, pl.ds(pl.multiple_of(q * rows, rows), rows), :] = bit_of(words, shift).astype(F32).astype(BF16)
        return 0

    lax.fori_loop(0, n, make_mask, 0)

    cs, cl = iota((2 * ants, LANES), 0), iota((2 * ants, LANES), 1)
    column_bits = []
    for s in range(subs):
        words = jnp.zeros((2 * ants, LANES), jnp.int32)
        for w in range(flags.shape[1]):
            here = (lax.div(cs, ants) * (LANES // WORD) + lax.div(cl, WORD)) == w
            words = jnp.where(here, flags[s, w], words)
        column_bits.append(bit_of(words, lax.rem(cl, WORD)))

    def place(c, q, again):
        t0, t1 = tiles[2 * q], tiles[2 * q + 1]
        at = pl.multiple_of(q * rows, rows)
        for p in range(parts):
            value = jnp.concatenate([vbuf[c][p, t0], vbuf[c][p, t1]], axis=0)
            for s in range(subs):
                piece = value[:, s * sub_len : (s + 1) * sub_len] * mask[s, pl.ds(at, rows), :]
                lanes = pl.ds(p * samples + s * sub_len, sub_len)
                x[c, pl.ds(at, rows), lanes] = piece
                if again:
                    x[c, pl.ds(pl.multiple_of(inputs + at, rows), rows), lanes] = piece

    for c in range(channels):
        v_copy(c).wait()
        lax.fori_loop(0, hops, lambda q, _: (place(c, q, True), 0)[1], 0, unroll=2)
        lax.fori_loop(hops, n, lambda q, _: (place(c, q, False), 0)[1], 0, unroll=2)

    def quarter(held):
        return jnp.concatenate([held, jnp.concatenate([held[:, samples:], -held[:, :samples]], axis=1)], axis=0)

    def destination(which, direction, s):
        step = (hops - s) * (1 - 2 * which) * (1 - 2 * direction)
        return wrap(z + step)

    def window_chip(which, chip):
        return wrap(chip - which * (hops - 1))

    def add_channel(which, direction, s, c, main):
        chip = destination(which, direction, s)
        ch = which * half_ch + c
        held = x[ch, pl.ds(pl.multiple_of(chip * rows, rows), rows), :]
        start = window_chip(which, chip) * rows
        wide = x[ch, pl.ds(pl.multiple_of(start, rows), window), :]
        main[direction, s, c * group : (c + 1) * group, :] = dot_nt(quarter(held), wide)

    def add_extra(which, direction, s, extra):
        chip = destination(which, direction, s)
        total = jnp.zeros((rows, half_ch * group), F32)
        for c in range(half_ch):
            ch = which * half_ch + c
            held = x[ch, pl.ds(pl.multiple_of(chip * rows, rows), rows), :]
            far = quarter(x[ch, pl.ds(pl.multiple_of(wrap(chip + hops) * rows, rows), rows), :])
            pieces = [far]
            if c:
                pieces.insert(0, jnp.zeros((c * group, far.shape[1]), BF16))
            if c < half_ch - 1:
                pieces.append(jnp.zeros(((half_ch - 1 - c) * group, far.shape[1]), BF16))
            total += dot_nt(held, jnp.concatenate(pieces, axis=0))
        extra[direction, s, 0:rows, :] = total
        t = tiles[2 * chip + which]
        shift = lax.rem(t, per_word) * ants + lax.rem(cs, ants)
        pairs = jnp.zeros((2 * ants, LANES), jnp.int32)
        for k in range(subs):
            words = jnp.zeros((2 * ants, LANES), jnp.int32) + flags[k, lax.div(t, per_word)]
            pairs += bit_of(words, shift) * column_bits[k]
        extra[direction, s, rows : rows + 2 * ants, :] = (pairs * sub_len).astype(F32)

    def sib_copies(direction, s):
        return [
            pltpu.make_async_remote_copy(
                src_ref=src.at[direction, s], dst_ref=dst.at[direction, s],
                send_sem=sib_send.at[direction, s, k], recv_sem=sib_recv.at[direction, s, k],
                device_id=sibling, device_id_type=MESH,
            )
            for k, (src, dst) in enumerate(((snd_m, sib_m), (snd_e, sib_e)))
        ]

    def send_sibling(direction, s):
        for copy in sib_copies(direction, s):
            copy.start()

    def whole(which, direction, s, main, extra):
        for c in range(half_ch):
            add_channel(which, direction, s, c, main)
        add_extra(which, direction, s, extra)

    def slot(direction, s, k):
        if k < half_ch:
            return [r.at[direction, s, pl.ds(k * group, group), :] for r in (ring_m, own_m, sib_m)]
        return [r.at[direction, s] for r in (ring_e, own_e, sib_e)]

    def ring_copy(direction, s, k):
        return pltpu.make_async_remote_copy(
            src_ref=slot(direction, s, k)[0], dst_ref=slot(direction, s + 1, k)[0],
            send_sem=ring_send.at[direction, k], recv_sem=ring_recv.at[direction, s + 1, k],
            device_id=ahead[direction], device_id_type=MESH,
        )

    def relay(direction, s, k, first):
        if not first:
            ring_copy(direction, s - 1, k).wait_recv()
        if k == 0 or k == half_ch:
            sib_copies(direction, s)[min(k, 1)].wait_recv()
        held, mine, theirs = slot(direction, s, k)
        if first:
            held[...] = mine[...] + theirs[...]
        else:
            held[...] = held[...] + (mine[...] + theirs[...])
            ring_copy(direction, s - 1, k).wait_send()
        ring_copy(direction, s, k).start()

    pl.semaphore_wait(barrier, 3)

    whole(other, 0, 0, snd_m, snd_e)
    send_sibling(0, 0)
    whole(core, 0, 0, own_m, own_e)

    def early(direction, _):
        whole(other, direction, 1, snd_m, snd_e)
        send_sibling(direction, 1)
        whole(core, direction, 1, own_m, own_e)
        return 0

    for k in range(half_ch + 1):
        relay(0, 0, k, True)
    lax.fori_loop(0, 2, early, 0)

    def one_hot(q, _):
        first = window_chip(core, z)
        chip = jnp.where(q < hops, wrap(first + q), wrap(z - sigma * (q - hops + 1)))
        t0, t1 = tiles[2 * chip], tiles[2 * chip + 1]
        wide_row, wide_lane = iota((rows, inputs), 0), iota((rows, inputs), 1)
        goal = jnp.where(wide_row < block, t0, t1) * block + lax.rem(wide_row, block)
        onehot[pl.ds(pl.multiple_of(q * rows, rows), rows), :] = jnp.where(wide_lane == goal, 1.0, 0.0).astype(BF16)
        return 0

    def step(s, first, last):
        directions = (0,) if first == 0 else (0, 1)
        ahead_of = s + 2
        for k in range(half_ch):
            for d in directions:
                relay(d, s, k, d == first)
            for d in range(last):
                add_channel(other, d, ahead_of, k, snd_m)
                add_channel(core, d, ahead_of, k, own_m)
        for d in directions:
            relay(d, s, half_ch, d == first)
        for d in range(last):
            add_extra(other, d, ahead_of, snd_e)
            send_sibling(d, ahead_of)
            add_extra(core, d, ahead_of, own_e)

    def ahead_only(direction, _):
        whole(other, direction, 2, snd_m, snd_e)
        send_sibling(direction, 2)
        whole(core, direction, 2, own_m, own_e)
        return 0

    lax.fori_loop(0, 2, ahead_only, 0)
    step(1, 1, 2)
    lax.fori_loop(0, n, one_hot, 0)
    lax.fori_loop(2, hops - 2, lambda s, _: (step(s, None, 2), 0)[1], 0)
    step(hops - 2, None, 1)
    step(hops - 1, None, 0)

    for copy in sib_copies(0, hops):
        copy.wait_recv()
    for d in range(2):
        for k in range(half_ch + 1):
            ring_copy(d, hops - 1, k).wait_recv()
    near = ring_m[0, hops] + ring_m[1, hops] + (own_m[0, hops] + sib_m[0, hops])
    extra = ring_e[0, hops] + ring_e[1, hops] + (own_e[0, hops] + sib_e[0, hops])
    turned[...] = near.T.reshape(hops, rows, half_ch * group)

    def exchange(d):
        slab = jnp.where(core == 0, d, hops - 1 - d)
        return pltpu.make_async_remote_copy(
            src_ref=turned.at[slab], dst_ref=exch.at[d - 1],
            send_sem=exch_send.at[d - 1], recv_sem=exch_recv.at[d - 1],
            device_id=device(wrap(z + sigma * d), core), device_id_type=MESH,
        )

    for d in range(hops - 1, 0, -1):
        exchange(d).start()

    def replaced(value, at):
        total = None
        for _ in range(3):
            part = value.astype(BF16)
            value = value - part.astype(F32)
            moved = jnp.dot(part, onehot[at : at + window, :], preferred_element_type=F32)
            total = moved if total is None else total + moved
        return total

    result = replaced(near, 0)
    for d in range(1, hops):
        exchange(d).wait_recv()
    blocks = [exch[d] for d in range(hops - 1)] + [extra[0:rows]]
    pairs = half_ch * parts
    mirrored = []
    for g in range(hops // pairs):
        mirrored.append(swap_chunks(blocks[g * pairs : (g + 1) * pairs], rows))
    far = []
    for k in range(pairs):
        line = jnp.concatenate([m[k] for m in mirrored], axis=1)
        far.append(-line if k % parts else line)
    result = result + replaced(jnp.concatenate(far, axis=0), window)
    for k in range(pairs):
        for t in range(2):
            final[t, k] = result[k * rows + t * block : k * rows + (t + 1) * block]

    finish = pltpu.make_async_remote_copy(
        src_ref=final.at[other], dst_ref=arrived, send_sem=fin_send, recv_sem=fin_recv,
        device_id=sibling, device_id_type=MESH,
    )
    finish.start()

    counts = extra[rows : rows + 2 * ants]
    out_row = iota((block, LANES), 0)
    spread_row, spread_col = iota((LANES, 2 * LANES), 0), iota((LANES, 2 * LANES), 1)
    spread = jnp.where(lax.div(spread_col, 2) == spread_row, 1.0, 0.0).astype(BF16)
    wide = []
    for h in range(2):
        picked = jnp.zeros((block, LANES), F32)
        for a in range(ants):
            line = counts[h * ants + a : h * ants + a + 1, :]
            picked = jnp.where(lax.div(out_row, 2) == a, jnp.broadcast_to(line, picked.shape), picked)
        wide.append(jnp.dot(picked.astype(BF16), spread, preferred_element_type=F32))
    divisor = jnp.maximum(jnp.concatenate(wide, axis=1)[:, :inputs], 1.0)

    for k in range(pairs):
        out[core * pairs + k] = final[core, k] / divisor
    finish.wait()
    for k in range(pairs):
        out[other * pairs + k] = arrived[k] / divisor

    for d in range(1, hops):
        exchange(d).wait_send()
    for d in range(2):
        for k in range(half_ch + 1):
            ring_copy(d, hops - 1, k).wait_send()

    def sent(s, _):
        for d in range(2):
            for copy in sib_copies(d, s):
                copy.wait_send()
        return 0

    for copy in sib_copies(0, 0) + sib_copies(0, hops):
        copy.wait_send()
    lax.fori_loop(1, hops, sent, 0)


def shards(n, voltages, antenna_flags, owned_tile):
    channels, parts, inputs, samples = voltages.shape
    tiles = owned_tile.shape[0]
    block = inputs // tiles
    rows = 2 * block
    hops = n // 2
    window = hops * rows
    half = channels // 2
    lanes = half * parts * rows
    extra = rows + block
    subs = antenna_flags.shape[0]
    slots = hops + 1
    dma = pltpu.SemaphoreType.DMA
    main_slots = pltpu.VMEM((2, slots, lanes, window), F32)
    extra_slots = pltpu.VMEM((2, slots, extra, lanes), F32)
    smem = pl.BlockSpec(memory_space=pltpu.SMEM)
    summed = pl.pallas_call(
        functools.partial(kernel, n),
        out_shape=jax.ShapeDtypeStruct((channels * parts, block, inputs), F32),
        in_specs=[smem, smem, pl.BlockSpec(memory_space=pl.ANY)],
        out_specs=pl.BlockSpec(memory_space=pltpu.VMEM),
        scratch_shapes=[
            *[pltpu.VMEM((parts, tiles, block, samples), BF16)] * channels,
            pltpu.VMEM((subs, inputs, LANES), BF16),
            pltpu.VMEM((channels, inputs + window, parts * samples), BF16),
            pltpu.VMEM((inputs, inputs), BF16),
            main_slots, extra_slots,
            main_slots, extra_slots,
            main_slots, extra_slots,
            main_slots, extra_slots,
            pltpu.VMEM((hops, rows, lanes), F32),
            pltpu.VMEM((hops - 1, rows, lanes), F32),
            pltpu.VMEM((2, half * parts, block, inputs), F32),
            pltpu.VMEM((half * parts, block, inputs), F32),
            dma((channels,)),
            dma((2, half + 1)),
            dma((2, slots, half + 1)),
            dma((2, slots, 2)),
            dma((2, slots, 2)),
            dma((hops - 1,)),
            dma((hops - 1,)),
            dma,
            dma,
        ],
        compiler_params=pltpu.CompilerParams(
            collective_id=0, has_side_effects=True, vmem_limit_bytes=60 * 1024 * 1024
        ),
    )(owned_tile, antenna_flags, voltages.reshape(channels, parts, tiles, block, samples))
    return summed.reshape(channels, parts, block, inputs).transpose(2, 0, 1, 3)


def solution(mesh):
    in_specs = (P("band", None, None, "tm"), P("tm", "band"), P())
    out_specs = P("tm", "band", None, None)
    return jax.shard_map(
        functools.partial(shards, mesh.shape["tm"] // 2),
        mesh=mesh, in_specs=in_specs, out_specs=out_specs, check_vma=False,
    )
```
